128 devices in a mesh: grp: 4 (over y, x), seq: 32 (over z, core).
Axes of the slice: x: 2, y: 2, z: 16, core: 2. Of those that a mesh axis runs over, the one named last changes fastest.
The devices are a block of a 8x8x16 slice.
Arguments:
- queries: bfloat16 [2048, 4096], P(('grp', 'seq')), parts along dimension 0, may hold values from -36 to 36
- new_keys: bfloat16 [2048, 1024], P(('grp', 'seq')), parts along dimension 0, may hold values from -24 to 24
- new_values: bfloat16 [2048, 1024], P(('grp', 'seq')), parts along dimension 0, may hold values from -12 to 12
- suffix_keys: bfloat16 [2048, 256, 1024], P(('grp', 'seq')), parts along dimension 0, may hold values from -18 to 18
- suffix_values: bfloat16 [2048, 256, 1024], P(('grp', 'seq')), parts along dimension 0, may hold values from -12 to 12
- suffix_lens: int32 [2048], P(('grp', 'seq')), parts along dimension 0, may hold values from 1 to 256, 65536 in all
- prefix_keys: bfloat16 [8192, 16, 1024], P(('grp', 'seq')), parts along dimension 0, may hold values from -12 to 12
- prefix_values: bfloat16 [8192, 16, 1024], P(('grp', 'seq')), parts along dimension 0, may hold values from -12 to 12
- page_table: int32 [8, 1024], P('grp'), parts along dimension 0, may hold values from 0 to 2047, as said below
- prefix_id: int32 [2048], P('grp'), parts along dimension 0, may hold values from 0 to 1
Outputs:
- attn_out: bfloat16 [2048, 4096], P(('grp', 'seq')), parts along dimension 0
The draws below stay inside these ranges and needn't reach their ends.
There are 4 independent parts, one for each index of `grp`. The reference program is written for one: setup_inputs(seed, part) draws one part's arguments, and reference() takes and returns one part's arrays. A program takes and returns all parts, laid end to end along the dimension named above; each array names one. Nothing has to cross between parts.
Inputs may be any that keep to these rules, and one draw needn't show every extreme that they name: `page_table`: every page id 0 to 2047 stands exactly once in the table. Each run of 64 page ids that starts at a multiple of 64 holds at least one page of every prefix.
All inputs are finite; a program needn't handle non-finite values. No bound on the sum of `suffix_lens` on one device may be relied on, other than what follows from the above.
Results may differ from the reference program's by a relative error of at most 0.005.
Values may be sent and summed in bfloat16 or wider, within the bound.
No kernel may reach another device: no remote copies, remote signals or barrier semaphores. Data moves between devices by JAX's collectives and lax.ppermute only.
A program may use at most 192 MiB of HBM per device.

```python
import math
import jax
import jax.numpy as jnp
import numpy as np
from jax import lax

H = 32
KV = 8
HD = 128
NPREF = 2
PAGE = 16
PAGES_DEV = 64
B_DEV = 16
SUF = 256
B = 512
PAGES = 2048
PPP = 1024
N_SEQ = 32


def shared_keys(key):
    raw_keys = 4.0 * jax.random.normal(jax.random.fold_in(key, 11), (B, KV * HD), jnp.float32)
    return jnp.clip(raw_keys, -24.0, 24.0)


def draw_new_keys(key, part):
    return shared_keys(key).astype(jnp.bfloat16)


def draw_queries(key, part):
    plain_draw = jnp.clip(jax.random.normal(jax.random.fold_in(key, 12), (B, H * HD), jnp.float32), -6.0, 6.0)
    return plain_draw.astype(jnp.bfloat16)


def draw_page_table(key, part):
    owner_count = PAGES // PAGES_DEV
    spare_slots = PAGES_DEV - NPREF
    leftover = jnp.repeat(jnp.arange(NPREF, dtype=jnp.int32), PPP - owner_count)
    leftover = jax.random.permutation(jax.random.fold_in(key, 3), leftover).reshape(owner_count, spare_slots)
    base_rows = jnp.tile(jnp.arange(NPREF, dtype=jnp.int32)[None, :], (owner_count, 1))
    labels = jnp.concatenate([base_rows, leftover], axis=1)
    labels = jax.random.permutation(jax.random.fold_in(key, 4), labels, axis=1, independent=True)
    order_list = jnp.argsort(labels.reshape(-1), stable=True)
    return order_list.reshape(NPREF, PPP).astype(jnp.int32)


def set_ends(drawn, stream_key, smallest, high):
    dims = drawn.shape
    spot = [jax.random.randint(jax.random.fold_in(stream_key, axis), (), 0, dims[axis]) for axis in range(len(dims))]
    drawn = drawn.at[tuple(spot)].set(smallest)
    longest = dims.index(max(dims))
    spot[longest] = (spot[longest] + 1) % dims[longest]
    return drawn.at[tuple(spot)].set(high)


def block_levels(key, dims, cuts, least, high):
    loudness, own = 1.0, jax.random.fold_in(key, 6)
    for dim, parts in cuts:
        draws = jnp.exp(jax.random.uniform(jax.random.fold_in(own, dim), (parts,), jnp.float32, least / len(cuts), high / len(cuts)))
        loudness = loudness * jnp.repeat(draws, dims[dim] // parts).reshape([-1 if axis == dim else 1 for axis in range(len(dims))])
    return loudness


def rank_bounds(number_of, skew):
    loads = [(1 << 20) // math.isqrt(standing ** skew) + 1 for standing in range(1, number_of + 1)]
    deviation = 1 + sum(loads) // (1 << 30)
    return np.cumsum(np.array([max(1, weight // deviation) for weight in loads]))


def ranked_ids(rng, extent, count, skew):
    table = rank_bounds(count, skew)
    lot = jax.random.randint(jax.random.fold_in(rng, 1), extent, 0, int(table[count - 1]))
    rank = jnp.searchsorted(jnp.asarray(table, jnp.int32), lot, side="right")
    return jax.random.permutation(jax.random.fold_in(rng, 2), count)[rank].astype(jnp.int32)


def split_up(count, total, most, skew):
    loads = [(1 << 20) // math.isqrt(standing ** skew) + 1 for standing in range(2, count + 1)]
    spare, counts = total - most - (count - 1), [1] * (count - 1)
    while spare > 0:
        free = [i for i in range(count - 1) if counts[i] < most]
        whole, remaining = sum([loads[i] for i in free]), spare
        for i in free:
            extra = min(most - counts[i], max(1, remaining * loads[i] // whole), spare)
            counts[i] = counts[i] + extra
            spare = spare - extra
    return np.array([most] + counts)


def ragged_sizes(key, count, total, reach, lean):
    if count == 2:
        one = jax.random.randint(key, (), max(1, total - reach), min(reach, total - 1) + 1)
        return jnp.stack([one, total - one])
    tallies = jnp.asarray(split_up(count, total, reach, lean), jnp.int32)
    couples = (count - 1) // 2
    source_of, taker = tallies[1:1 + 2 * couples:2], tallies[2:2 + 2 * couples:2]
    room = jnp.minimum(source_of - 1, reach - taker)
    shifted = jax.random.randint(jax.random.fold_in(key, 1), (couples,), 0, 1 << 20) % (room + 1)
    tallies = tallies.at[1:1 + 2 * couples:2].set(source_of - shifted).at[2:2 + 2 * couples:2].set(taker + shifted)
    return tallies[jax.random.permutation(jax.random.fold_in(key, 2), count)]


def gaussian(rng, dims, width, limit, pieces=(), kind=jnp.bfloat16):
    array = jax.random.normal(rng, dims, jnp.float32) * width
    if len(pieces) > 0:
        array = block_levels(rng, dims, pieces, -0.22, 0.18) * array
    return jnp.clip(array, min=-limit, max=limit).astype(kind)


def setup_inputs(seed: int = 0, part: int = 0) -> dict:
    key_list = jax.random.split(jax.random.key(seed), 11)
    part_splits = jax.random.split(jax.random.fold_in(key_list[10], part), 11)
    return {
        "queries": draw_queries(jax.random.fold_in(jax.random.fold_in(key_list[10], part), 71), part),
        "new_keys": draw_new_keys(jax.random.fold_in(jax.random.fold_in(key_list[10], part), 71), part),
        "new_values": gaussian(part_splits[2], (B, KV * HD), 2.0, 12.0, ((0, 32),)),
        "suffix_keys": gaussian(part_splits[3], (B, SUF, KV * HD), 3.0, 18.0, ((0, 32),)),
        "suffix_values": gaussian(part_splits[4], (B, SUF, KV * HD), 2.0, 12.0, ((0, 32),)),
        "suffix_lens": ragged_sizes(part_splits[5], B, B * SUF // 2, SUF, 2).astype(jnp.int32),
        "prefix_keys": gaussian(part_splits[6], (PAGES, PAGE, KV * HD), 2.0, 12.0, ((0, 32),)),
        "prefix_values": gaussian(part_splits[7], (PAGES, PAGE, KV * HD), 2.0, 12.0, ((0, 32),)),
        "page_table": draw_page_table(jax.random.fold_in(jax.random.fold_in(key_list[10], part), 71), part),
        "prefix_id": set_ends(ranked_ids(part_splits[9], (B,), NPREF, 2), jax.random.fold_in(part_splits[9], 3), 0, NPREF - 1).astype(jnp.int32),
    }


def reference(queries, new_keys, new_values, suffix_keys, suffix_values, suffix_lens, prefix_keys, prefix_values, page_table, prefix_id):
    group_size = H // KV
    softmax_scale = 1.0 / math.sqrt(HD)
    block_tokens = PAGES_DEV * PAGE
    page_ids = jnp.arange(PAGES, dtype=jnp.int32)
    page_hits = jnp.any(page_table[:, :, None] == page_ids[None, None, :], axis=1)
    prefix_of_page = lax.optimization_barrier(jnp.sum(page_hits.astype(jnp.int32) * jnp.arange(NPREF, dtype=jnp.int32)[:, None], axis=0))
    token_label = jnp.repeat(prefix_of_page, PAGE)
    pool_keys = prefix_keys.reshape(PAGES * PAGE, KV, HD).astype(jnp.float32)
    pool_values = prefix_values.reshape(N_SEQ, block_tokens, KV, HD).astype(jnp.float32)
    block_count = B // B_DEV
    slot_index = jnp.arange(SUF, dtype=jnp.int32)

    def one_block(inputs):
        block_queries, block_new_keys, block_new_values, block_suffix_keys, block_suffix_values, block_lens, block_ids = inputs
        query_head_count = block_queries.reshape(B_DEV, KV, group_size, HD).astype(jnp.float32)
        prefix_scores = jnp.einsum('bkgd,tkd->bkgt', query_head_count, pool_keys) * softmax_scale
        prefix_live = (block_ids[:, None] == token_label[None, :])[:, None, None, :]
        prefix_scores = jnp.where(prefix_live, prefix_scores, -1e+30)
        prefix_scores = prefix_scores.reshape(B_DEV, KV, group_size, N_SEQ, block_tokens)
        prefix_live = prefix_live.reshape(B_DEV, 1, 1, N_SEQ, block_tokens)
        block_peak = lax.optimization_barrier(jnp.max(prefix_scores, axis=4))
        block_weights = jnp.where(prefix_live, jnp.exp(prefix_scores - block_peak[..., None]), 0.0)
        block_mass = lax.optimization_barrier(jnp.sum(block_weights, axis=4))
        block_round = lax.optimization_barrier(block_weights.astype(jnp.bfloat16)).astype(jnp.float32)
        block_numer = jnp.einsum('bkgot,otkd->bkgod', block_round, pool_values)
        block_out = block_numer / block_mass[..., None]
        block_out = lax.optimization_barrier(block_out.astype(jnp.bfloat16)).astype(jnp.float32)
        block_lse = block_peak + jnp.log(block_mass)
        own_keys = block_suffix_keys.reshape(B_DEV, SUF, KV, HD).astype(jnp.float32)
        own_values = block_suffix_values.reshape(B_DEV, SUF, KV, HD).astype(jnp.float32)
        suffix_scores = jnp.einsum('bkgd,btkd->bkgt', query_head_count, own_keys) * softmax_scale
        suffix_live = (slot_index[None, :] < block_lens[:, None])[:, None, None, :]
        suffix_scores = jnp.where(suffix_live, suffix_scores, -1e+30)
        incoming_keys = block_new_keys.reshape(B_DEV, KV, HD).astype(jnp.float32)
        incoming_values = block_new_values.reshape(B_DEV, KV, HD).astype(jnp.float32)
        incoming_scores = jnp.einsum('iqnc,iqc->iqn', query_head_count, incoming_keys) * softmax_scale
        home_peak = jnp.maximum(lax.optimization_barrier(jnp.max(suffix_scores, axis=3)), incoming_scores)
        suffix_weights = jnp.where(suffix_live, jnp.exp(suffix_scores - home_peak[..., None]), 0.0)
        fresh_weights = jnp.exp(incoming_scores - home_peak)
        home_mass = lax.optimization_barrier(jnp.sum(suffix_weights, axis=3)) + fresh_weights
        suffix_round = lax.optimization_barrier(suffix_weights.astype(jnp.bfloat16)).astype(jnp.float32)
        incoming_rounded = lax.optimization_barrier(fresh_weights.astype(jnp.bfloat16)).astype(jnp.float32)
        resident_numerator = jnp.einsum('bkgt,btkd->bkgd', suffix_round, own_values)
        resident_numerator = resident_numerator + jnp.einsum('cqx,cqh->cqxh', incoming_rounded, incoming_values)
        home_out = resident_numerator / home_mass[..., None]
        home_lse = home_peak + jnp.log(home_mass)
        overall = jnp.maximum(lax.optimization_barrier(jnp.max(block_lse, axis=3)), home_lse)
        factor = jnp.exp(block_lse - overall[..., None])
        home_factor = jnp.exp(home_lse - overall)
        merged = lax.optimization_barrier(jnp.sum(factor[..., None] * block_out, axis=3)) + home_factor[..., None] * home_out
        divisor = lax.optimization_barrier(jnp.sum(factor, axis=3)) + home_factor
        result = merged / divisor[..., None]
        return result.reshape(B_DEV, H * HD).astype(jnp.bfloat16)
    stacked = (queries.reshape(block_count, B_DEV, H * HD), new_keys.reshape(block_count, B_DEV, KV * HD), new_values.reshape(block_count, B_DEV, KV * HD), suffix_keys.reshape(block_count, B_DEV, SUF, KV * HD), suffix_values.reshape(block_count, B_DEV, SUF, KV * HD), suffix_lens.reshape(block_count, B_DEV), prefix_id.reshape(block_count, B_DEV))
    outputs = lax.map(one_block, stacked)
    return outputs.reshape(B, H * HD)
```

```python
import functools
import math

import jax
import jax.numpy as jnp
from jax import lax
from jax.experimental import pallas as pl
from jax.experimental.pallas import tpu as pltpu
from jax.sharding import Mesh
from jax.sharding import PartitionSpec as P


H = 32
KV = 8
HD = 128
NPREF = 2
G = H // KV
CORES = 2
KVC = KV // CORES
ROWS = 128
EXT = 16
LOG2E = math.log2(math.e)
SCALE2 = LOG2E / math.sqrt(HD)
BIG = float(2**20)
GRP_SEQ = ("grp", "z", "c")
F32 = jnp.float32
BF16 = jnp.bfloat16

floor_score = -1e30


def store_lse(ref, lses):
    row = lax.broadcasted_iota(jnp.int32, (EXT, ROWS), 0)
    ext = jnp.zeros((EXT, ROWS), F32)
    for g, lse in enumerate(lses):
        hi = lse.astype(BF16).astype(F32)
        rest = lse - hi
        mid = rest.astype(BF16).astype(F32)
        for i, term in enumerate((hi, mid, rest - mid)):
            ext = jnp.where(row == 3 * g + i, term, ext)
    ref[KVC * HD :, :] = ext.astype(BF16)


def load_packed(ref, g):
    ext = ref[KVC * HD :, :].astype(F32)[3 * g : 3 * g + 3]
    return ref[g * HD : (g + 1) * HD, :].astype(F32), ext[0:1] + (ext[1:2] + ext[2:3])


def merged(parts):
    peak = functools.reduce(jnp.maximum, [lse for _, lse in parts])
    weights = [jnp.exp2(lse - peak) for _, lse in parts]
    total = sum(weights[1:], weights[0])
    inv = 1.0 / total
    out = sum(((w * inv) * out for w, (out, _) in zip(weights, parts)), 0.0)
    return out, peak + jnp.log2(total)


def prepare_kernel(c_ref, k1_ref, k2_ref, v1_ref, v2_ref, k_ref, v_ref):
    del c_ref
    tokens = k1_ref.shape[0]
    k_ref[0, :tokens] = k1_ref[...]
    k_ref[0, tokens:] = k2_ref[...]
    v_ref[0, :HD, :tokens] = v1_ref[...].T
    v_ref[0, :HD, tokens:] = v2_ref[...].T
    row = lax.broadcasted_iota(jnp.int32, (EXT, 2 * tokens), 0)
    v_ref[0, HD:, :] = jnp.where(row == 0, 1.0, 0.0).astype(BF16)


def prepare(c, keys, values):
    tokens = keys[0].shape[0]
    kv_spec = pl.BlockSpec((tokens, HD), lambda g, c_ref: (0, c_ref[0] * KVC + g))
    return pl.pallas_call(
        prepare_kernel,
        out_shape=(
            jax.ShapeDtypeStruct((KVC, CORES * tokens, HD), BF16),
            jax.ShapeDtypeStruct((KVC, HD + EXT, CORES * tokens), BF16),
        ),
        grid_spec=pltpu.PrefetchScalarGridSpec(
            num_scalar_prefetch=1,
            grid=(KVC,),
            in_specs=[kv_spec] * 4,
            out_specs=[
                pl.BlockSpec((1, CORES * tokens, HD), lambda g, c_ref: (g, 0, 0)),
                pl.BlockSpec((1, HD + EXT, CORES * tokens), lambda g, c_ref: (g, 0, 0)),
            ],
        ),
        compiler_params=pltpu.CompilerParams(vmem_limit_bytes=16 * 2**20),
        cost_estimate=pl.CostEstimate(flops=2 * 10**9, bytes_accessed=8 * KVC * tokens * HD * 2, transcendentals=0),
        name="prepare",
    )(c, *keys, *values)


def attn_kernel(step, block, qa_ref, qb_ref, qm_ref, km_ref, k_ref, v_ref, oa_ref, ob_ref):
    half = qa_ref.shape[0] // 2
    tokens = k_ref.shape[1]
    nt = (((1,), (1,)), ((), ()))
    nn = (((1,), (0,)), ((), ()))
    lses = []
    for g in range(KVC):
        q = jnp.concatenate(
            [
                r[h * half : (h + 1) * half, (g * G + j) * HD : (g * G + j + 1) * HD]
                for r in (qa_ref, qb_ref)
                for h in range(CORES)
                for j in range(G)
            ],
            axis=0,
        )
        qx = jnp.concatenate([q, qm_ref[step - 1]], axis=1)
        scores, peaks = [], []
        for t in range(0, tokens, block):
            kx = jnp.concatenate([k_ref[g, t : t + block], km_ref[t : t + block]], axis=1)
            s = lax.dot_general(kx, qx, nt, preferred_element_type=F32)
            scores.append(s)
            peaks.append(jnp.max(s.reshape(-1, 64, 2 * ROWS), axis=0))
        peak = jnp.max(functools.reduce(jnp.maximum, peaks), axis=0, keepdims=True) * SCALE2
        total = None
        for i, s in enumerate(scores):
            p = jnp.exp2(s * SCALE2 - peak).astype(BF16)
            part = lax.dot_general(v_ref[g, :, i * block : (i + 1) * block], p, nn, preferred_element_type=F32)
            total = part if total is None else total + part
        mass = total[HD : HD + 1]
        out = (total[:HD] * (1.0 / mass)).astype(BF16)
        oa_ref[g * HD : (g + 1) * HD, :] = out[:, :ROWS]
        ob_ref[g * HD : (g + 1) * HD, :] = out[:, ROWS:]
        lses.append(peak + jnp.log2(mass))
    store_lse(oa_ref, [x[:, :ROWS] for x in lses])
    store_lse(ob_ref, [x[:, ROWS:] for x in lses])


def attend(step, qa, qb, qmask, kmask, keys, values):
    tokens = keys.shape[1]
    vmem = pl.BlockSpec(memory_space=pltpu.VMEM)
    o_type = jax.ShapeDtypeStruct((KVC * HD + EXT, ROWS), BF16)
    pairs = KVC * tokens * 2 * ROWS
    return pl.pallas_call(
        functools.partial(attn_kernel, step, 256),
        out_shape=(o_type, o_type),
        in_specs=[vmem] * 6,
        out_specs=(vmem, vmem),
        compiler_params=pltpu.CompilerParams(vmem_limit_bytes=24 * 2**20),
        cost_estimate=pl.CostEstimate(flops=pairs * 3 * HD * 2, bytes_accessed=KVC * 2 * tokens * HD * 2, transcendentals=pairs),
        name="attend",
    )(qa, qb, qmask, kmask, keys, values)


def merge_kernel(n, *refs):
    for i in range(n):
        lses = []
        for g in range(KVC):
            out, lse = merged([load_packed(refs[2 * i], g), load_packed(refs[2 * i + 1], g)])
            refs[2 * n + i][g * HD : (g + 1) * HD, :] = out.astype(BF16)
            lses.append(lse)
        store_lse(refs[2 * n + i], lses)


def merge_pairs(*pairs):
    n = len(pairs)
    flat = [x for pair in pairs for x in pair]
    vmem = pl.BlockSpec(memory_space=pltpu.VMEM)
    return pl.pallas_call(
        functools.partial(merge_kernel, n),
        out_shape=tuple(jax.ShapeDtypeStruct(flat[0].shape, BF16) for _ in range(n)),
        in_specs=[vmem] * (2 * n),
        out_specs=tuple([vmem] * n),
        compiler_params=pltpu.CompilerParams(vmem_limit_bytes=12 * 2**20),
        cost_estimate=pl.CostEstimate(flops=10**9, bytes_accessed=3 * n * flat[0].size * 2, transcendentals=0),
        name="merge",
    )(*flat)


def collect_kernel(n, *refs):
    out_ref = refs[n]
    row = lax.broadcasted_iota(jnp.int32, (8, ROWS), 0)
    for g in range(KVC):
        out, lse = merged([load_packed(refs[i], g) for i in range(n)])
        out_ref[g, :HD, :] = out
        out_ref[g, HD:, :] = jnp.where(row == 0, lse, 0.0)


def collect(*parts):
    vmem = pl.BlockSpec(memory_space=pltpu.VMEM)
    return pl.pallas_call(
        functools.partial(collect_kernel, len(parts)),
        out_shape=jax.ShapeDtypeStruct((KVC, HD + 8, ROWS), F32),
        in_specs=[vmem] * len(parts),
        out_specs=vmem,
        compiler_params=pltpu.CompilerParams(vmem_limit_bytes=12 * 2**20),
        name="collect",
    )(*parts)


def final_kernel(c_ref, mine_ref, other_ref, home_ref, lse_ref, o_ref):
    half = ROWS // 2
    seqs = half // G
    first = c_ref[0] == 0
    for g in range(KVC):
        m_out = mine_ref[g, :HD, :].T[:half]
        o_out = other_ref[g, :HD, :].T[half:]
        m_lse = jnp.broadcast_to(mine_ref[g, HD : HD + 1, :], (HD, ROWS)).T[:half]
        o_lse = jnp.broadcast_to(other_ref[g, HD : HD + 1, :], (HD, ROWS)).T[half:]
        low = (jnp.where(first, m_out, o_out), jnp.where(first, m_lse, o_lse))
        high = (jnp.where(first, o_out, m_out), jnp.where(first, o_lse, m_lse))
        for k, part in ((g, low), (KVC + g, high)):
            out, _ = merged([part, (home_ref[k], lse_ref[k])])
            for j in range(G):
                at = (k * G + j) * HD
                o_ref[:, at : at + HD] = out[j * seqs : (j + 1) * seqs].astype(o_ref.dtype)


def finish(c, mine, other, home_out, home_lse, rows):
    vmem = pl.BlockSpec(memory_space=pltpu.VMEM)
    return pl.pallas_call(
        final_kernel,
        out_shape=jax.ShapeDtypeStruct((rows, H * HD), BF16),
        in_specs=[pl.BlockSpec(memory_space=pltpu.SMEM), vmem, vmem, vmem, vmem],
        out_specs=vmem,
        compiler_params=pltpu.CompilerParams(vmem_limit_bytes=12 * 2**20),
        name="finish",
    )(c, mine, other, home_out, home_lse)


def home_part(queries, new_keys, new_values, suffix_keys, suffix_values, suffix_lens):
    local_rows = queries.shape[0]
    softmax_scale = 1.0 / math.sqrt(HD)
    resident_heads = queries.reshape(local_rows, KV, G, HD)
    slot_count = suffix_keys.shape[1]
    own_keys = suffix_keys.reshape(local_rows, slot_count, KV, HD)
    own_values = suffix_values.reshape(local_rows, slot_count, KV, HD)
    suffix_scores = jnp.einsum("bkgd,btkd->bkgt", resident_heads, own_keys, preferred_element_type=F32) * softmax_scale
    live = (jnp.arange(slot_count, dtype=jnp.int32)[None, :] < suffix_lens[:, None])[:, None, None, :]
    suffix_scores = jnp.where(live, suffix_scores, floor_score)
    suffix_peak = jnp.max(suffix_scores, axis=3)
    incoming_keys = new_keys.reshape(local_rows, KV, HD)
    incoming_values = new_values.reshape(local_rows, KV, HD)
    incoming_scores = jnp.einsum("iqnc,iqc->iqn", resident_heads, incoming_keys, preferred_element_type=F32) * softmax_scale
    home_peak = jnp.maximum(suffix_peak, incoming_scores)
    suffix_weights = jnp.where(live, jnp.exp(suffix_scores - home_peak[..., None]), 0.0)
    fresh_weights = jnp.exp(incoming_scores - home_peak)
    home_mass = jnp.sum(suffix_weights, axis=3) + fresh_weights
    numerator = jnp.einsum("bkgt,btkd->bkgd", suffix_weights.astype(BF16), own_values, preferred_element_type=F32)
    numerator = numerator + jnp.einsum("cqx,cqh->cqxh", fresh_weights.astype(BF16), incoming_values, preferred_element_type=F32)
    home_out = numerator / home_mass[..., None]
    home_lse = (home_peak + jnp.log(home_mass)) * LOG2E
    rows = G * local_rows
    home_out = home_out.transpose(1, 2, 0, 3).reshape(KV, rows, HD)
    home_lse = home_lse.transpose(1, 2, 0).reshape(KV, rows)
    return home_out, jnp.broadcast_to(home_lse[..., None], (KV, rows, HD))


def attention(
    queries,
    new_keys,
    new_values,
    suffix_keys,
    suffix_values,
    suffix_lens,
    prefix_keys,
    prefix_values,
    page_table,
    prefix_id,
):
    rows = queries.shape[0]
    chips = lax.axis_size("z")
    reach = chips // 2
    z = lax.axis_index("z")
    c = lax.axis_index("c")
    c_arr = c.astype(jnp.int32).reshape(1)
    pages_dev, page = prefix_keys.shape[:2]
    tokens = pages_dev * page
    swap = [(0, 1), (1, 0)]

    def shift(x, by):
        return lax.ppermute(x, "z", [(i, (i + by) % chips) for i in range(chips)])

    def side(x):
        mid = x.shape[1] // 2
        return jnp.where(c == 0, x[:, :mid], x[:, mid:])

    q_other = lax.ppermute(queries, "c", swap)
    keys = prefix_keys.reshape(tokens, KV * HD)
    values = prefix_values.reshape(tokens, KV * HD)
    keys = (keys, lax.ppermute(keys, "c", swap))
    values = (values, lax.ppermute(values, "c", swap))
    q_chip = jnp.concatenate([side(queries), side(q_other)], axis=0)

    device = z * CORES + jnp.stack([c, 1 - c])
    page_ids = (device[:, None] * pages_dev + jnp.arange(pages_dev, dtype=jnp.int32)[None, :]).reshape(-1)
    hits = jnp.any(page_table[:, :, None] == page_ids[None, None, :], axis=1)
    label = jnp.sum(hits.astype(jnp.int32) * jnp.arange(NPREF, dtype=jnp.int32)[:, None], axis=0)
    lane = jnp.arange(HD, dtype=jnp.int32)
    page_mask = jnp.where((lane[None, :] < NPREF) & (lane[None, :] != label[:, None]), -1.0, 0.0).astype(BF16)
    kmask = jnp.broadcast_to(page_mask[:, None, :], (CORES * pages_dev, page, HD)).reshape(CORES * tokens, HD)
    ids = prefix_id.reshape(chips, CORES, rows)
    ids = jnp.where(c == 0, ids, ids[:, ::-1])
    steps = jnp.arange(1, reach + 1, dtype=jnp.int32)
    source = jnp.stack([(z - steps) % chips, jnp.where(steps == reach, z, (z + steps) % chips)], axis=1)
    pick = source[:, :, None] == jnp.arange(chips, dtype=jnp.int32)[None, None, :]
    chosen = jnp.sum(jnp.where(pick[..., None, None], ids[None, None], 0), axis=2)
    chosen = jnp.broadcast_to(chosen[:, :, :, None, :], (reach, 2, CORES, G, rows)).reshape(reach, 2 * ROWS)
    qmask = jnp.where(chosen[..., None] == lane[None, None, :], BIG, 0.0).astype(BF16)

    keys, values = prepare(c_arr, keys, values)
    up = down = q_chip
    above, below = {}, {}
    for k in range(1, reach + 1):
        up = shift(up, 1)
        if k < reach:
            down = shift(down, -1)
        above[k], below[k] = attend(k, up, down if k < reach else q_chip, qmask, kmask, keys, values)
    own = below.pop(reach)

    mid = reach // 2
    far_a, near_a = above[reach], above[mid]
    far_b, near_b = below[reach - 1], below[mid]
    for i in range(1, mid):
        near_a, near_b = shift(near_a, -1), shift(near_b, 1)
        far_b = shift(far_b, 1 if i < mid - 1 else reach - mid + 1)
        far_a = shift(far_a, -1)
        pairs = [(far_a, above[reach - i]), (near_a, above[mid - i]), (near_b, below[mid - i])]
        if i < mid - 1:
            far_a, near_a, near_b, far_b = merge_pairs(*pairs, (far_b, below[reach - 1 - i]))
        else:
            far_a, near_a, near_b = merge_pairs(*pairs)
    near_a, near_b = shift(near_a, -1), shift(near_b, 1)
    far_a = shift(far_a, -(mid + 1))
    mine = collect(own, far_b, near_a, near_b, far_a)
    other = lax.ppermute(mine, "c", swap)
    home_out, home_lse = home_part(queries, new_keys, new_values, suffix_keys, suffix_values, suffix_lens)
    return finish(c_arr, mine, other, home_out, home_lse, rows)


def solution(mesh):
    finer = Mesh(mesh.devices.reshape(mesh.shape["grp"], mesh.shape["seq"] // CORES, CORES), GRP_SEQ)
    placed = (
        P(GRP_SEQ, None),
        P(GRP_SEQ, None),
        P(GRP_SEQ, None),
        P(GRP_SEQ, None, None),
        P(GRP_SEQ, None, None),
        P(GRP_SEQ),
        P(GRP_SEQ, None, None),
        P(GRP_SEQ, None, None),
        P("grp", None),
        P("grp"),
    )
    return jax.shard_map(attention, mesh=finer, in_specs=placed, out_specs=P(GRP_SEQ, None), check_vma=False)
```
